32 devices in a mesh: dp: 4 (over y, x), seq: 4 (over z), grp: 2 (over core).
Axes of the slice: x: 2, y: 2, z: 4, core: 2. Of those that a mesh axis runs over, the one named last changes fastest.
Arguments:
- text_proj: bfloat16 [3, 16, 12, 128, 128], P(None, 'dp', None, ('seq', 'grp')), may hold values from -50 to 50
- image_proj: bfloat16 [3, 16, 12, 160, 128], P(None, ('dp', 'seq'), None, 'grp'), may hold values from -50 to 50
- text_grad: bfloat16 [16, 12, 128, 128], P('dp', None, ('seq', 'grp')), may hold values from -15 to 15
- image_grad: bfloat16 [16, 12, 160, 128], P(('dp', 'seq'), None, 'grp'), may hold values from -15 to 15
- text_lengths: int32 [16], P(('dp', 'seq')), may hold values from 1 to 128
- norm_gains: float32 [2, 2, 128], replicated, may hold values from 0.7 to 5.2
Outputs:
- text_out: bfloat16 [16, 12, 128, 128], P('dp', None, ('seq', 'grp'))
- image_out: bfloat16 [16, 12, 160, 128], P(('dp', 'seq'), None, 'grp')
- text_proj_grad: bfloat16 [3, 16, 12, 128, 128], P(None, 'dp', None, ('seq', 'grp'))
- image_proj_grad: bfloat16 [3, 16, 12, 160, 128], P(None, ('dp', 'seq'), None, 'grp')
- gain_grad: float32 [2, 2, 128], replicated
The draws below stay inside these ranges and needn't reach their ends.
All inputs are finite; a program needn't handle non-finite values.
Results may differ from the reference program's by a relative error of at most 0.025.
The reference program's roundings to bfloat16 on the way (of `normed`, `rounded_probs`, `grad_value`, `grad_scores` and `grad_normed`) count: a program that leaves them out, or rounds other values in their place, can miss the bound.
Values may be sent and summed in bfloat16 or wider, within the bound.
No kernel may reach another device: no remote copies, remote signals or barrier semaphores. Data moves between devices by JAX's collectives and lax.ppermute only.
A program may use at most 64 MiB of HBM per device.

```python
import math
import jax
import jax.numpy as jnp
from jax import lax

HEADS = 12
HD = 128
TXT = 128
IMG = 160
SAMPLES = 16
JOINT = 288


def scaled_noise(key, shape):
    noise_key, scale_key = jax.random.split(key)
    values = jax.random.truncated_normal(noise_key, -5.0, 5.0, shape, jnp.float32)
    row_scale = jnp.exp(jax.random.uniform(scale_key, shape[:-1] + (1,), jnp.float32, 0.0, math.log(10.0)))
    component = jnp.arange(3).reshape(3, 1, 1, 1, 1)
    return values * jnp.where(component < 2, row_scale, 1.0)


def draw_text_proj(key, part):
    values = scaled_noise(jax.random.fold_in(key, 11), (3, SAMPLES, HEADS, TXT, HD))
    return values.astype(jnp.bfloat16)


def draw_image_proj(key, part):
    noise_key = jax.random.fold_in(jax.random.fold_in(key, 13), 0)
    values = scaled_noise(noise_key, (3, SAMPLES, HEADS, IMG, HD))
    return values.astype(jnp.bfloat16)


def ramped(key, shape, offset):
    values = jax.random.truncated_normal(key, -4.0, 4.0, shape, jnp.float32)
    along_samples = 1.0 + 2.0 * jnp.arange(SAMPLES, dtype=jnp.float32) / max(SAMPLES - 1, 1)
    along_positions = 1.0 + 2.0 * (offset + jnp.arange(shape[2], dtype=jnp.float32)) / (JOINT - 1)
    return values * 0.4 * along_samples[:, None, None, None] * along_positions[None, None, :, None]


def draw_text_grad(key, part):
    return ramped(jax.random.fold_in(key, 23), (SAMPLES, HEADS, TXT, HD), 0).astype(jnp.bfloat16)


def draw_image_grad(key, part):
    return ramped(jax.random.fold_in(key, 29), (SAMPLES, HEADS, IMG, HD), TXT).astype(jnp.bfloat16)


def draw_norm_gains(key, part):
    gain_key = jax.random.fold_in(key, 37)
    return jnp.exp(jax.random.uniform(gain_key, (2, 2, HD), jnp.float32, math.log(0.7), math.log(1.5)))


def with_ends(entries, rng, low, top_value):
    dims = entries.shape
    index_at = [jax.random.randint(jax.random.fold_in(rng, axis), (), 0, dims[axis]) for axis in range(len(dims))]
    entries = entries.at[tuple(index_at)].set(low)
    longest = dims.index(max(dims))
    index_at[longest] = (index_at[longest] + 1) % dims[longest]
    return entries.at[tuple(index_at)].set(top_value)


def setup_inputs(seed: int = 0) -> dict:
    seeds = jax.random.split(jax.random.key(seed), 7)
    text_proj = draw_text_proj(jax.random.fold_in(seeds[6], 71), 0)
    image_proj = draw_image_proj(jax.random.fold_in(seeds[6], 71), 0)
    text_grad = draw_text_grad(jax.random.fold_in(seeds[6], 71), 0)
    image_grad = draw_image_grad(jax.random.fold_in(seeds[6], 71), 0)
    text_lengths = with_ends(jax.random.randint(seeds[4], (SAMPLES,), 1, TXT + 1), jax.random.fold_in(seeds[4], 1), 1, TXT).astype(jnp.int32)
    norm_gains = draw_norm_gains(jax.random.fold_in(seeds[6], 71), 0)
    return dict(text_proj=text_proj, image_proj=image_proj, text_grad=text_grad, image_grad=image_grad, text_lengths=text_lengths, norm_gains=norm_gains)


EPSILON = 1e-06
MASKED = -1e+30

def normalize(raw_vals, is_text, norm_gains):
    inverse = lax.rsqrt(lax.optimization_barrier(jnp.mean(raw_vals * raw_vals, axis=-1, keepdims=True)) + EPSILON)
    unit_vec = raw_vals * inverse
    gain_map = jnp.where(is_text[None, :, None], norm_gains[0][:, None, :], norm_gains[1][:, None, :])
    return (unit_vec, inverse, gain_map)

def forward(queries, key_rows, value_rows, key_valid):
    factor = queries.shape[-1] ** (-0.5)
    scores = jnp.einsum('nqd,nkd->nqk', queries.astype(jnp.float32), key_rows.astype(jnp.float32)) * factor
    scores = jnp.where(key_valid[:, None, :], scores, MASKED)
    row_max = lax.optimization_barrier(jnp.max(scores, axis=-1, keepdims=True))
    exponent = jnp.exp(scores - row_max)
    attn_probs = exponent / lax.optimization_barrier(jnp.sum(exponent, axis=-1, keepdims=True))
    rounded_probs = attn_probs.astype(jnp.bfloat16)
    attn_local = jnp.einsum('nqk,nkd->nqd', rounded_probs.astype(jnp.float32), value_rows.astype(jnp.float32))
    return (attn_probs, rounded_probs, attn_local)

def backward(queries, key_rows, value_rows, attn_probs, rounded_probs, grad_out):
    factor = queries.shape[-1] ** (-0.5)
    grad_value = jnp.einsum('nqk,nqd->nkd', rounded_probs.astype(jnp.float32), grad_out.astype(jnp.float32)).astype(jnp.bfloat16)
    grad_probs = jnp.einsum('nqd,nkd->nqk', grad_out.astype(jnp.float32), value_rows.astype(jnp.float32))
    row_delta = lax.optimization_barrier(jnp.sum(attn_probs * grad_probs, axis=-1, keepdims=True))
    grad_scores = (attn_probs * (grad_probs - row_delta) * factor).astype(jnp.bfloat16)
    grad_query = jnp.einsum('nqk,nkd->nqd', grad_scores.astype(jnp.float32), key_rows.astype(jnp.float32)).astype(jnp.bfloat16)
    grad_key = jnp.einsum('nqk,nqd->nkd', grad_scores.astype(jnp.float32), queries.astype(jnp.float32)).astype(jnp.bfloat16)
    return (grad_query, grad_key, grad_value)

def reference(text_proj, image_proj, text_grad, image_grad, text_lengths, norm_gains):
    joint_len = TXT + IMG
    position = jnp.arange(joint_len, dtype=jnp.int32)
    is_text = position < TXT
    text_flag = is_text.astype(jnp.float32)

    def per_sample(sample_item):
        text_block, image_block, text_cot, image_cot, text_length = sample_item
        sample_block = jnp.concatenate([text_block, image_block], axis=2)
        cotangent = jnp.concatenate([text_cot, image_cot], axis=1)
        raw_vals = sample_block[:2].astype(jnp.float32)
        unit_vec, inverse, gain_map = normalize(raw_vals, is_text, norm_gains)
        normed = (unit_vec * gain_map[:, None]).astype(jnp.bfloat16)
        key_valid = (position >= TXT) | (position < text_length)
        key_valid = jnp.broadcast_to(key_valid[None, :], (sample_block.shape[1], joint_len))
        attn_probs, rounded_probs, attn_local = forward(normed[0], normed[1], sample_block[2], key_valid)
        grad_query, grad_key, grad_value = backward(normed[0], normed[1], sample_block[2], attn_probs, rounded_probs, cotangent)
        grad_normed = jnp.stack([grad_query, grad_key]).astype(jnp.float32)
        per_position = lax.optimization_barrier(jnp.sum(grad_normed * unit_vec, axis=1))
        gain_part = jnp.stack([jnp.einsum('l,qld->qd', text_flag, per_position), jnp.einsum('l,qld->qd', 1.0 - text_flag, per_position)])
        grad_unit = grad_normed * gain_map[:, None]
        grad_raw = inverse * (grad_unit - unit_vec * lax.optimization_barrier(jnp.mean(grad_unit * unit_vec, axis=-1, keepdims=True)))
        gradients = jnp.concatenate([grad_raw.astype(jnp.bfloat16), grad_value[None]], axis=0)
        attn_rounded = attn_local.astype(jnp.bfloat16)
        return (attn_rounded[:, :TXT], attn_rounded[:, TXT:], gradients[:, :, :TXT], gradients[:, :, TXT:], gain_part)
    text_out, image_out, text_grads, image_grads, gain_parts = lax.map(per_sample, (jnp.moveaxis(text_proj, 1, 0), jnp.moveaxis(image_proj, 1, 0), text_grad, image_grad, text_lengths))
    gain_grad = lax.optimization_barrier(jnp.sum(gain_parts, axis=0)) / text_proj.shape[1]
    return (text_out, image_out, jnp.moveaxis(text_grads, 0, 1), jnp.moveaxis(image_grads, 0, 1), gain_grad)
```

```python
import functools
import math
import jax
import jax.numpy as jnp
from jax import lax
from jax.experimental import pallas as pl
from jax.experimental.pallas import tpu as pltpu
from jax.sharding import PartitionSpec as P

TXT = 128


EPSILON = 1e-06
MASKED = -1e30


def forward(queries, key_rows, value_rows, key_valid):
    factor = queries.shape[-1] ** (-0.5)
    scores = (
        jnp.einsum("nqd,nkd->nqk", queries, key_rows, preferred_element_type=jnp.float32) * factor
    )
    scores = jnp.where(key_valid[:, None, :], scores, MASKED)
    row_max = jnp.max(scores, axis=-1, keepdims=True)
    exponent = jnp.exp(scores - row_max)
    attn_probs = exponent / jnp.sum(exponent, axis=-1, keepdims=True)
    rounded_probs = attn_probs.astype(jnp.bfloat16)
    attn_local = jnp.einsum(
        "nqk,nkd->nqd", rounded_probs, value_rows, preferred_element_type=jnp.float32
    )
    return (attn_probs, rounded_probs, attn_local)


def backward_terms(queries, key_rows, value_rows, attn_probs, rounded_probs, grad_out):
    factor = queries.shape[-1] ** (-0.5)
    grad_value = jnp.einsum(
        "nqk,nqd->nkd", rounded_probs, grad_out, preferred_element_type=jnp.float32
    )
    grad_probs = jnp.einsum(
        "nqd,nkd->nqk", grad_out, value_rows, preferred_element_type=jnp.float32
    )
    row_delta = jnp.sum(attn_probs * grad_probs, axis=-1, keepdims=True)
    grad_scores = (attn_probs * (grad_probs - row_delta) * factor).astype(jnp.bfloat16)
    grad_query = jnp.einsum(
        "nqk,nkd->nqd", grad_scores, key_rows, preferred_element_type=jnp.float32
    ).astype(jnp.bfloat16)
    grad_key = jnp.einsum("nqk,nqd->nkd", grad_scores, queries, preferred_element_type=jnp.float32)
    return (grad_query, grad_key, grad_value)


def sums_item(packed):
    query_one, key_one, value_one, valid_one, grad_one = packed
    attn_probs, rounded_probs, attn_local = forward(
        query_one[None], key_one[None], value_one[None], valid_one[None]
    )
    grad_query, grad_key, grad_value = backward_terms(
        query_one[None], key_one[None], value_one[None], attn_probs, rounded_probs, grad_one[None]
    )
    return (attn_local[0].astype(jnp.bfloat16), grad_query[0], grad_key[0], grad_value[0])


def whole_item(packed):
    attn_local, grad_query, grad_key, grad_value = sums_item(packed)
    return (attn_local, grad_query, grad_key.astype(jnp.bfloat16), grad_value.astype(jnp.bfloat16))


def unit_parts(raw_bf):
    raw_vals = raw_bf.astype(jnp.float32)
    inverse = lax.rsqrt(jnp.mean(raw_vals * raw_vals, axis=-1, keepdims=True) + EPSILON)
    return (raw_vals * inverse, inverse)


def raw_gradient(grad_normed_bf, unit_vec, inverse, gain_rows):
    grad_normed = grad_normed_bf.astype(jnp.float32)
    gain_part = jnp.sum(grad_normed * unit_vec, axis=(1, 2, 3))
    grad_unit = grad_normed * gain_rows
    grad_raw = inverse * (
        grad_unit - unit_vec * jnp.mean(grad_unit * unit_vec, axis=-1, keepdims=True)
    )
    return (grad_raw.astype(jnp.bfloat16), gain_part)


def global_position(local_row, owner_index, text_rows, text_group, image_rows, grp_count):
    text_place = (
        local_row // text_group * grp_count + owner_index
    ) * text_group + local_row % text_group
    image_place = TXT + owner_index * image_rows + (local_row - text_rows)
    return jnp.where(local_row < text_rows, text_place, image_place)


def gathered(text_proj, image_proj, text_grad, image_grad, text_lengths, norm_gains):
    seq_count = lax.axis_size("seq")
    grp_count = lax.axis_size("grp")
    sample_count, head_count, image_rows, head_size = image_grad.shape
    text_group = text_proj.shape[3]
    text_rows = text_group * seq_count
    local_len = text_rows + image_rows
    text_unit, text_inverse = unit_parts(text_proj[:2])
    image_unit, image_inverse = unit_parts(image_proj[:2])
    text_gain = norm_gains[0][:, None, None, None, :]
    image_gain = norm_gains[1][:, None, None, None, :]
    text_stack = jnp.concatenate(
        [(text_unit * text_gain).astype(jnp.bfloat16), text_proj[2:]], axis=0
    )
    image_stack = jnp.concatenate(
        [(image_unit * image_gain).astype(jnp.bfloat16), image_proj[2:]], axis=0
    )
    text_here, text_cot = (
        lax.all_to_all(text_stack, "seq", split_axis=1, concat_axis=3, tiled=True),
        lax.all_to_all(text_grad[None], "seq", split_axis=1, concat_axis=3, tiled=True),
    )
    joint_rows = jnp.concatenate([text_here, image_stack], axis=3)
    cotangent_rows = jnp.concatenate([text_cot[0], image_grad], axis=2)
    key_row = jnp.arange(local_len * grp_count, dtype=jnp.int32)
    key_place = global_position(
        key_row % local_len, key_row // local_len, text_rows, text_group, image_rows, grp_count
    )
    key_valid = (key_place[None, :] >= TXT) | (key_place[None, :] < text_lengths[:, None])
    full_len = local_len * grp_count
    moved_rows, moved_cot = (
        lax.all_to_all(joint_rows, "grp", split_axis=2, concat_axis=3, tiled=True),
        lax.all_to_all(cotangent_rows[None], "grp", split_axis=2, concat_axis=3, tiled=True),
    )
    head_share = moved_rows.shape[2]
    item_count = sample_count * head_share
    flat_rows = moved_rows.reshape(3, item_count, full_len, head_size)
    item_valid = jnp.broadcast_to(
        key_valid[:, None, :], (sample_count, head_share, full_len)
    ).reshape(item_count, full_len)
    attn_local, grad_query, grad_key, grad_value = lax.map(
        whole_item,
        (
            flat_rows[0],
            flat_rows[1],
            flat_rows[2],
            item_valid,
            moved_cot.reshape(item_count, full_len, head_size),
        ),
    )
    results = jnp.stack([attn_local, grad_query, grad_key, grad_value]).reshape(
        4, sample_count, head_share, full_len, head_size
    )
    placed = lax.all_to_all(results, "grp", split_axis=3, concat_axis=2, tiled=True)
    text_back = lax.all_to_all(
        placed[:, :, :, :text_rows], "seq", split_axis=3, concat_axis=1, tiled=True
    )
    image_back = placed[:, :, :, text_rows:]
    text_raw, text_part = raw_gradient(text_back[1:3], text_unit, text_inverse, text_gain)
    image_raw, image_part = raw_gradient(image_back[1:3], image_unit, image_inverse, image_gain)
    partial_value = jnp.stack([text_part, image_part])
    summed_gain = lax.psum(partial_value, ("dp", "seq", "grp"))
    gain_grad = summed_gain / (sample_count * lax.axis_size("dp") * seq_count)
    text_proj_grad = jnp.concatenate([text_raw, text_back[3:]], axis=0)
    image_proj_grad = jnp.concatenate([image_raw, image_back[3:]], axis=0)
    return (text_back[0], image_back[0], text_proj_grad, image_proj_grad, gain_grad)


LOG2E = math.log2(math.e)
SUBLANES = 16


def xor_pairs(count, step):
    return [(index, index ^ step) for index in range(count)]


def peer_list(seq_count, grp_count):
    half = max(seq_count // 2, 1)
    steps = [step for step in range(half, seq_count)] + [step for step in range(1, half)]
    remote = [(step, core) for step in steps for core in range(grp_count)]
    near = [(0, core) for core in range(1, grp_count)]
    return [(0, 0)] + remote + near


def swap(value, step, core):
    grp_count = lax.axis_size("grp")
    if step == 0:
        return lax.ppermute(value, "grp", xor_pairs(grp_count, core))
    count = lax.axis_size("seq") * grp_count
    return lax.ppermute(value, ("seq", "grp"), xor_pairs(count, step * grp_count + core))


def pack_body(peers, head_share, chunk_heads, place, text_proj, text_grad, image_proj, image_grad, *rest):
    chunks = head_share // chunk_heads
    n_text = len(peers) * chunks
    text_out, rest = rest[:n_text], rest[n_text:]
    image_out, sems = rest[:-1], rest[-1]
    seq_at, grp_at = place[0], place[1]
    copies = []
    for chunk in range(chunks):
        for at, (step, core) in enumerate(peers):
            sample = seq_at ^ step
            heads = pl.ds((grp_at ^ core) * head_share + chunk * chunk_heads, chunk_heads)
            target = text_out[chunk * len(peers) + at]
            copies.append((text_proj.at[:, sample, heads], target.at[pl.ds(0, 3)]))
            copies.append((text_grad.at[sample, heads], target.at[3]))
    for core, target in enumerate(image_out):
        heads = pl.ds((grp_at ^ core) * head_share, head_share)
        copies.append((image_proj.at[:, 0, heads], target.at[pl.ds(0, 3)]))
        copies.append((image_grad.at[0, heads], target.at[3]))
    started = [
        pltpu.make_async_copy(source, target, sems.at[at])
        for at, (source, target) in enumerate(copies)
    ]
    for copy in started:
        copy.start()
    for copy in started:
        copy.wait()


def unpack_body(peers, head_share, chunk_heads, place, *refs):
    chunks = head_share // chunk_heads
    n_text = len(peers) * chunks
    text_in, refs = refs[:n_text], refs[n_text:]
    image_in, outs = refs[:-5], refs[-5:]
    text_out, image_out, text_grad, image_grad, sems = outs
    seq_at, grp_at = place[0], place[1]
    copies = []
    for core, source in enumerate(image_in):
        heads = pl.ds((grp_at ^ core) * head_share, head_share)
        copies.append((source.at[0], image_out.at[0, heads]))
        copies.append((source.at[pl.ds(1, 3)], image_grad.at[:, 0, heads]))
    for chunk in range(chunks):
        for at, (step, core) in enumerate(peers):
            sample = seq_at ^ step
            heads = pl.ds((grp_at ^ core) * head_share + chunk * chunk_heads, chunk_heads)
            source = text_in[chunk * len(peers) + at]
            copies.append((source.at[0], text_out.at[sample, heads]))
            copies.append((source.at[pl.ds(1, 3)], text_grad.at[:, sample, heads]))
    started = [
        pltpu.make_async_copy(source, target, sems.at[at])
        for at, (source, target) in enumerate(copies)
    ]
    for copy in started:
        copy.start()
    for copy in started:
        copy.wait()


def matmul(left, right, left_dim, right_dim):
    return lax.dot_general(
        left, right, (((left_dim,), (right_dim,)), ((), ())), preferred_element_type=jnp.float32
    )


def attend_body(n_text, head_base, heads, place, gains, *refs):
    text_in, refs = refs[:n_text], refs[n_text:]
    image_in, refs = refs[:2], refs[2:]
    text_out, refs = refs[:n_text], refs[n_text:]
    image_out, gain_out, gain_sum = refs[:2], refs[2], refs[3]
    group = text_in[0].shape[2]
    image_rows = image_in[0].shape[2]
    text_len = n_text * group
    size = text_in[0].shape[3]
    factor = size ** (-0.5)
    length = place[2]
    row = lax.broadcasted_iota(jnp.int32, (group, 1), 0)
    bias = jnp.concatenate(
        [
            jnp.where(row + place[3 + at] * group < length, 0.0, -1e30).astype(jnp.float32)
            for at in range(n_text)
        ],
        axis=0,
    )
    gain_rows = [[gains[stream, c][None, :] for stream in range(2)] for c in range(2)]
    gain_sum[...] = jnp.zeros_like(gain_sum)

    def per_stream(values, which):
        return jnp.concatenate(
            [values[:text_len] * which[0], values[text_len:] * which[1]], axis=0
        )

    def head(at, carry):
        def gather(tensor):
            return jnp.concatenate(
                [piece[tensor, at] for piece in text_in]
                + [piece[tensor, head_base + at] for piece in image_in],
                axis=0,
            )

        def norm(c):
            raw = gather(c).astype(jnp.float32)
            inverse = lax.rsqrt(jnp.mean(raw * raw, axis=-1, keepdims=True) + EPSILON)
            unit = raw * inverse
            return unit, inverse, per_stream(unit, gain_rows[c]).astype(jnp.bfloat16)

        query_unit, query_inverse, query = norm(0)
        key_unit, key_inverse, key = norm(1)
        value = gather(2)
        cotangent = gather(3)
        scores = matmul(key, query, 1, 1) * (factor * LOG2E)
        scores = jnp.concatenate([scores[:text_len] + bias, scores[text_len:]], axis=0)
        exponent = jnp.exp2(scores - jnp.max(scores, axis=0, keepdims=True))
        probs = exponent * (1.0 / jnp.sum(exponent, axis=0, keepdims=True))
        rounded = probs.astype(jnp.bfloat16)
        grad_probs = matmul(value, cotangent, 1, 1)
        delta = jnp.sum(probs * grad_probs, axis=0, keepdims=True)
        grad_scores = (probs * (grad_probs - delta) * factor).astype(jnp.bfloat16)

        def scatter(tensor, values):
            for piece_at, piece in enumerate(text_out):
                piece[tensor, at] = values[piece_at * group : (piece_at + 1) * group]
            for piece_at, piece in enumerate(image_out):
                start = text_len + piece_at * image_rows
                piece[tensor, head_base + at] = values[start : start + image_rows]

        scatter(0, matmul(rounded, value, 0, 0).astype(jnp.bfloat16))
        scatter(3, matmul(rounded, cotangent, 1, 0).astype(jnp.bfloat16))

        def raw_gradient(c, grad, unit, inverse):
            grad = grad.astype(jnp.bfloat16).astype(jnp.float32)
            product = grad * unit
            for stream, part in enumerate((product[:text_len], product[text_len:])):
                gain_sum[stream * 2 + c] += jnp.sum(part.reshape(-1, 8, size), axis=0)
            mean = jnp.mean(per_stream(product, gain_rows[c]), axis=-1, keepdims=True)
            result = inverse * (per_stream(grad, gain_rows[c]) - unit * mean)
            scatter(1 + c, result.astype(jnp.bfloat16))

        raw_gradient(0, matmul(grad_scores, key, 0, 0), query_unit, query_inverse)
        raw_gradient(1, matmul(grad_scores, query, 1, 0), key_unit, key_inverse)
        return carry

    lax.fori_loop(0, heads, head, 0)
    gain_out[...] = jnp.sum(gain_sum[...], axis=1)


def in_vmem():
    return pl.BlockSpec(memory_space=pltpu.VMEM)


def in_smem():
    return pl.BlockSpec(memory_space=pltpu.SMEM)


def anywhere():
    return pl.BlockSpec(memory_space=pl.ANY)


def tree_sum(values):
    while len(values) > 1:
        values = [values[at] + values[at + 1] for at in range(0, len(values), 2)]
    return values[0]


def total_gain(value):
    value = value + swap(value, 0, 1)
    for axis in ("dp", "seq"):
        count = lax.axis_size(axis)
        others = [lax.ppermute(value, axis, xor_pairs(count, step)) for step in range(1, count)]
        value = tree_sum([value] + others)
    return value


def direct(text_proj, image_proj, text_grad, image_grad, text_lengths, norm_gains):
    seq_count = lax.axis_size("seq")
    grp_count = lax.axis_size("grp")
    heads, size = image_grad.shape[1], image_grad.shape[3]
    group, image_rows = text_proj.shape[3], image_grad.shape[2]
    head_share = heads // grp_count
    chunk_heads = head_share
    peers = peer_list(seq_count, grp_count)
    n_text = len(peers)
    seq_at, grp_at = lax.axis_index("seq"), lax.axis_index("grp")
    sources = [(seq_at ^ step) * grp_count + (grp_at ^ core) for step, core in peers]
    place = jnp.stack([seq_at, grp_at, text_lengths[0]] + sources).astype(jnp.int32)
    text_piece = jax.ShapeDtypeStruct((4, chunk_heads, group, size), jnp.bfloat16)
    image_piece = jax.ShapeDtypeStruct((4, head_share, image_rows, size), jnp.bfloat16)
    packed = pl.pallas_call(
        functools.partial(pack_body, peers, head_share, chunk_heads),
        out_shape=[text_piece] * n_text + [image_piece] * grp_count,
        in_specs=[in_smem()] + [anywhere()] * 4,
        out_specs=[in_vmem()] * (n_text + grp_count),
        scratch_shapes=[pltpu.SemaphoreType.DMA((2 * (n_text + grp_count),))],
        name="pack",
    )(place, text_proj, text_grad, image_proj, image_grad)
    text_sent, image_sent = packed[:n_text], packed[n_text:]
    text_here = [text_sent[0]] + [
        swap(value, step, core) for value, (step, core) in zip(text_sent[1:], peers[1:])
    ]
    image_here = [image_sent[0], swap(image_sent[1], 0, 1)]
    attended = pl.pallas_call(
        functools.partial(attend_body, n_text, 0, chunk_heads),
        out_shape=[text_piece] * n_text
        + [image_piece] * grp_count
        + [jax.ShapeDtypeStruct((4, size), jnp.float32)],
        in_specs=[in_smem()] + [in_vmem()] * (1 + n_text + grp_count),
        out_specs=[in_vmem()] * (n_text + grp_count + 1),
        scratch_shapes=[pltpu.VMEM((4, 8, size), jnp.float32)],
        name="attend",
    )(place, norm_gains, *text_here, *image_here)
    text_done, image_done = attended[:n_text], attended[n_text : n_text + grp_count]
    text_back = [text_done[0]] + [
        swap(value, step, core) for value, (step, core) in zip(text_done[1:], peers[1:])
    ]
    image_back = [image_done[0], swap(image_done[1], 0, 1)]
    gain_sum = total_gain(attended[-1])
    gain_grad = gain_sum.reshape(2, 2, size) / (
        text_grad.shape[0] * lax.axis_size("dp")
    )
    outs = pl.pallas_call(
        functools.partial(unpack_body, peers, head_share, chunk_heads),
        out_shape=[
            jax.ShapeDtypeStruct(value.shape, jnp.bfloat16)
            for value in (text_grad, image_grad, text_proj, image_proj)
        ],
        in_specs=[in_smem()] + [in_vmem()] * (n_text + grp_count),
        out_specs=[anywhere()] * 4,
        scratch_shapes=[pltpu.SemaphoreType.DMA((2 * (n_text + grp_count),))],
        name="unpack",
    )(place, *text_back, *image_back)
    return (*outs, gain_grad)


def power_of_two(count):
    return count & (count - 1) == 0


def per_device(text_proj, image_proj, text_grad, image_grad, text_lengths, norm_gains):
    seq_count, grp_count = lax.axis_size("seq"), lax.axis_size("grp")
    aligned = text_proj.shape[3] % SUBLANES == 0 and image_proj.shape[3] % SUBLANES == 0
    fits = (
        aligned
        and grp_count == 2
        and seq_count <= 8
        and power_of_two(seq_count)
        and power_of_two(lax.axis_size("dp"))
        and image_grad.shape[0] == 1
        and image_grad.shape[1] % grp_count == 0
    )
    form = direct if fits else gathered
    return form(text_proj, image_proj, text_grad, image_grad, text_lengths, norm_gains)


def solution(mesh):
    placed = (
        P(None, "dp", None, ("seq", "grp"), None),
        P(None, ("dp", "seq"), None, "grp", None),
        P("dp", None, ("seq", "grp"), None),
        P(("dp", "seq"), None, "grp", None),
        P(("dp", "seq")),
        P(),
    )
    return jax.shard_map(
        per_device,
        mesh=mesh,
        in_specs=placed,
        out_specs=(
            P("dp", None, ("seq", "grp"), None),
            P(("dp", "seq"), None, "grp", None),
            P(None, "dp", None, ("seq", "grp"), None),
            P(None, ("dp", "seq"), None, "grp", None),
            P(),
        ),
        check_vma=False,
    )
```
